32 devices in a mesh: head: 8 (over z, core), kv: 4 (over y, x).
Axes of the slice: x: 2, y: 2, z: 4, core: 2. Of those that a mesh axis runs over, the one named last changes fastest.
Arguments:
- queries: bfloat16 [2048, 8192], P(('kv', 'head')), may hold values from -6 to 6
- key_rows: bfloat16 [2048, 1024], P(('kv', 'head')), may hold values from -6 to 6
- value_matrix: bfloat16 [2048, 1024], P(('kv', 'head')), may hold values from -6 to 6
- doc_ids: int32 [2048], P(('kv', 'head')), may hold values from 0 to 5, as said below
Outputs:
- attended: bfloat16 [2048, 8192], P(('kv', 'head'))
The draws below stay inside these ranges and needn't reach their ends.
Inputs may be any that keep to these rules, and one draw needn't show every extreme that they name: doc_ids starts at 0, never falls, and rises by one at the first token of each of the 6 documents; every document starts at an even position and has 2 tokens or more.
All inputs are finite; a program needn't handle non-finite values.
Results may differ from the reference program's by a relative error of at most 0.015.
Values may be sent and summed in bfloat16 or wider, within the bound.
A program may use at most 64 MiB of HBM per device.

```python
import math
import jax
import jax.numpy as jnp
from jax import lax

QUERY_HEADS = 64
KEY_VALUE_HEADS = 8
HEAD_SIZE = 128
DOCS = 6
SEQUENCE_TOKENS = 2048


def draw_queries(key, part):
    column_total = QUERY_HEADS * HEAD_SIZE
    drawn_values = jax.random.truncated_normal(jax.random.fold_in(key, 1), -6.0, 6.0, (SEQUENCE_TOKENS, column_total), jnp.float32)
    return drawn_values.astype(jnp.bfloat16)


def draw_key_rows(key, part):
    column_total = KEY_VALUE_HEADS * HEAD_SIZE
    drawn_values = jax.random.truncated_normal(jax.random.fold_in(key, 2), -6.0, 6.0, (SEQUENCE_TOKENS, column_total), jnp.float32)
    return drawn_values.astype(jnp.bfloat16)


def draw_doc_ids(key, part):
    pair_count = SEQUENCE_TOKENS // 2
    shuffled = jax.random.permutation(jax.random.fold_in(key, 11), pair_count - 1) + 1
    boundaries = 2 * shuffled[:DOCS - 1]
    positions = jnp.arange(SEQUENCE_TOKENS, dtype=jnp.int32)
    return jnp.sum((positions[:, None] >= boundaries[None, :]).astype(jnp.int32), axis=1).astype(jnp.int32)


def level_of(rng, shape, pieces, smallest, high):
    def one(dim, shards_of):
        draws = jax.random.uniform(jax.random.fold_in(jax.random.fold_in(rng, 6), dim), (shards_of,), jnp.float32, smallest / len(pieces), high / len(pieces))
        return jnp.repeat(jnp.exp(draws), shape[dim] // shards_of).reshape((-1,) + (1,) * (len(shape) - dim - 1))

    factor_of = one(*pieces[0])
    for cut in pieces[1:]:
        factor_of = factor_of * one(*cut)
    return factor_of


def noise(own_key, shape, width, reach, split=(), kind=jnp.bfloat16):
    level = level_of(own_key, shape, split, -0.22, 0.18) if split else 1.0
    drawn = jax.random.normal(own_key, shape, jnp.float32) * width * level
    return jnp.minimum(jnp.maximum(drawn, -reach), reach).astype(kind)


def setup_inputs(seed: int = 0) -> dict:
    splits = jax.random.split(jax.random.key(seed), 5)
    queries = draw_queries(jax.random.fold_in(splits[4], 71), 0)
    key_rows = draw_key_rows(jax.random.fold_in(splits[4], 71), 0)
    value_matrix = noise(splits[2], (SEQUENCE_TOKENS, KEY_VALUE_HEADS * HEAD_SIZE), 1.0, 6.0, ((0, 32),))
    doc_ids = draw_doc_ids(jax.random.fold_in(splits[4], 71), 0)
    return {"queries": queries, "key_rows": key_rows, "value_matrix": value_matrix, "doc_ids": doc_ids}


def reference(queries, key_rows, value_matrix, doc_ids):
    seq_len = queries.shape[0]
    queries_per_group = QUERY_HEADS // KEY_VALUE_HEADS
    block_rows = math.gcd(seq_len, 512)
    scale = HEAD_SIZE ** -0.5

    def single_group(key_value_head):
        head_keys = lax.dynamic_slice_in_dim(key_rows, key_value_head * HEAD_SIZE, HEAD_SIZE, 1).astype(jnp.float32)
        head_values = lax.dynamic_slice_in_dim(value_matrix, key_value_head * HEAD_SIZE, HEAD_SIZE, 1).astype(jnp.float32)
        group_queries = lax.dynamic_slice_in_dim(queries, key_value_head * queries_per_group * HEAD_SIZE, queries_per_group * HEAD_SIZE, 1)
        key_pos = jnp.arange(seq_len, dtype=jnp.int32)

        def one_block(block_index):
            first_row = (block_index * block_rows).astype(jnp.int32)
            rows_now = lax.dynamic_slice_in_dim(group_queries, first_row, block_rows, 0)
            rows_now = rows_now.astype(jnp.float32).reshape(block_rows, queries_per_group, HEAD_SIZE)
            query_pos = first_row + jnp.arange(block_rows, dtype=jnp.int32)
            query_doc = lax.dynamic_slice_in_dim(doc_ids, first_row, block_rows, 0)
            scores = jnp.einsum("rhd,cd->hrc", rows_now, head_keys, precision=lax.Precision.HIGHEST) * scale
            allowed = (key_pos[None, :] <= query_pos[:, None]) & (doc_ids[None, :] == query_doc[:, None])
            masked = jnp.where(allowed, scores, -1.0e30)
            row_max = jnp.max(masked, axis=-1)
            weights = jnp.where(allowed, jnp.exp(masked - row_max[..., None]), 0.0)
            row_sum = jnp.sum(weights, axis=-1)
            rounded = lax.optimization_barrier(weights.astype(jnp.bfloat16)).astype(jnp.float32)
            summed = jnp.einsum("hrc,cd->hrd", rounded, head_values, precision=lax.Precision.HIGHEST)
            result = summed / row_sum[..., None]
            return result.transpose(1, 0, 2).reshape(block_rows, queries_per_group * HEAD_SIZE).astype(jnp.bfloat16)

        blocks = lax.map(one_block, jnp.arange(seq_len // block_rows, dtype=jnp.int32))
        return blocks.reshape(seq_len, queries_per_group * HEAD_SIZE)

    group_total = lax.map(single_group, jnp.arange(KEY_VALUE_HEADS, dtype=jnp.int32))
    return group_total.transpose(1, 0, 2).reshape(seq_len, QUERY_HEADS * HEAD_SIZE)
```

```python
import functools
import math

import jax
import jax.numpy as jnp
from jax import lax
from jax.experimental import pallas as pl
from jax.experimental.pallas import tpu as pltpu
from jax.sharding import PartitionSpec as P

QUERY_HEADS = 64
KEY_VALUE_HEADS = 8
HEAD_SIZE = 128
CORES = 2
NEG_FILL = -1e30
SCALE_LOG2 = HEAD_SIZE ** -0.5 * math.log2(math.e)
MESH = pl.DeviceIdType.MESH


def peer_id(slot, level):
    return {"kv": slot // CORES, "head": level * CORES + slot % CORES}


def place():
    kv_here, head_here = lax.axis_index("kv"), lax.axis_index("head")
    return kv_here, head_here // CORES, lax.rem(head_here, CORES)


def gather_kernel(slots, levels, q_ref, k_ref, v_ref, d_ref, qo, ko, vo, do, sems):
    kv_here, level, core = place()
    me = kv_here * CORES + core
    width = q_ref.shape[1] // slots
    query_heads = width // HEAD_SIZE
    group = QUERY_HEADS // KEY_VALUE_HEADS
    slab_send, slab_recv, line_send, line_recv, own = sems

    barrier = pltpu.get_barrier_semaphore()
    for step in range(1, slots):
        peer = lax.rem(me + step, slots)
        pl.semaphore_signal(barrier, inc=1, device_id=peer_id(peer, level), device_id_type=MESH)

    @pl.when(level > 0)
    def _():
        pl.semaphore_signal(barrier, inc=1, device_id=peer_id(me, level - 1), device_id_type=MESH)

    @pl.when(level < levels - 1)
    def _():
        pl.semaphore_signal(barrier, inc=1, device_id=peer_id(me, level + 1), device_id_type=MESH)

    def parts(slot):
        kv_column = pl.multiple_of((slot * query_heads // group) * HEAD_SIZE, HEAD_SIZE)
        q_column = pl.multiple_of(slot * width, HEAD_SIZE)
        return (
            (k_ref.at[:, pl.ds(kv_column, HEAD_SIZE)], ko.at[kv_here, level, core]),
            (v_ref.at[:, pl.ds(kv_column, HEAD_SIZE)], vo.at[kv_here, level, core]),
            (d_ref, do.at[kv_here, level, core]),
            (q_ref.at[:, pl.ds(q_column, width)], qo.at[kv_here, core]),
        )

    local = [pltpu.make_async_copy(s, d, own.at[i]) for i, (s, d) in enumerate(parts(me))]
    for copy in local:
        copy.start()
    pl.semaphore_wait(
        barrier,
        slots - 1 + (level > 0).astype(jnp.int32) + (level < levels - 1).astype(jnp.int32),
    )

    def slab_copy(step, part):
        peer = lax.rem(me + step, slots)
        source, target = parts(peer)[part]
        return pltpu.make_async_remote_copy(
            src_ref=source, dst_ref=target,
            send_sem=slab_send.at[part, peer], recv_sem=slab_recv.at[part, me],
            device_id=peer_id(peer, level), device_id_type=MESH,
        )

    for part in range(4):
        for step in range(1, slots):
            slab_copy(step, part).start()

    def slab_wait(part, source):
        target = (
            ko.at[source // CORES, level, lax.rem(source, CORES)],
            vo.at[source // CORES, level, lax.rem(source, CORES)],
            do.at[source // CORES, level, lax.rem(source, CORES)],
            qo.at[source // CORES, lax.rem(source, CORES)],
        )[part]
        pltpu.make_async_remote_copy(
            src_ref=target, dst_ref=target,
            send_sem=slab_send.at[part, source], recv_sem=slab_recv.at[part, source],
            device_id=peer_id(source, level), device_id_type=MESH,
        ).wait_recv()

    buffers = (ko, vo, do)

    def line_copy(part, strip, slab, up):
        ref = buffers[part].at[strip, slab]
        return pltpu.make_async_remote_copy(
            src_ref=ref, dst_ref=ref,
            send_sem=line_send.at[part, strip, slab, 1 if up else 0],
            recv_sem=line_recv.at[part, strip, slab],
            device_id=peer_id(me, level + 1 if up else level - 1), device_id_type=MESH,
        )

    for copy in local:
        copy.wait()
    strips = slots // CORES

    def line_send_all(strip, slab, up, act):
        for part in range(3):
            copy = line_copy(part, strip, slab, up)
            copy.start() if act else copy.wait_send()

    for ahead in range(strips):
        strip = lax.rem(kv_here + ahead, strips)
        for source_core in range(CORES):
            source = strip * CORES + source_core

            @pl.when(source != me)
            def _():
                for part in range(3):
                    slab_wait(part, source)

        @pl.when(level < levels - 1)
        def _():
            line_send_all(strip, level, True, True)

        @pl.when(level > 0)
        def _():
            line_send_all(strip, level, False, True)

    for step in range(1, levels):
        for ahead in range(strips):
            strip = lax.rem(kv_here + ahead, strips)
            for up in (True, False):
                slab = level - step if up else level + step
                exists = (slab >= 0) if up else (slab < levels)
                onward = (level < levels - 1) if up else (level > 0)

                @pl.when(exists)
                def _():
                    for part in range(3):
                        line_copy(part, strip, slab, True).wait_recv()

                @pl.when(exists & onward)
                def _():
                    line_send_all(strip, slab, up, True)

    for step in range(0, levels):
        for strip in range(strips):
            for up in (True, False):
                slab = level - step if up else level + step
                exists = (slab >= 0) if up else (slab < levels)
                onward = (level < levels - 1) if up else (level > 0)

                @pl.when(exists & onward)
                def _():
                    line_send_all(strip, slab, up, False)

    for step in range(1, slots):
        slab_wait(3, lax.rem(me + step, slots))
    for part in range(4):
        for step in range(1, slots):
            slab_copy(step, part).wait_send()


def attend_kernel(levels, heads, tokens, span, docs_ref, q_ref, k_ref, v_ref, d_ref, o_ref, acc):
    strips = q_ref.shape[0]
    rows = CORES * tokens
    level = lax.axis_index("head") // CORES
    pairs = heads // 2
    chunk = span // rows
    blocks = k_ref.shape[0] // span

    def one_strip(strip, carry):
        own_chunk = strip * levels + level
        first_doc = docs_ref[own_chunk * CORES, 0]
        high = own_chunk // chunk + 1

        def count(block, low):
            last = docs_ref[(block + 1) * chunk * CORES - 1, rows - 1]
            return low + jnp.where(last < first_doc, 1, 0)

        low = lax.fori_loop(0, high - 1, count, 0)
        acc[...] = jnp.zeros_like(acc)
        own_docs = d_ref[own_chunk * CORES] + d_ref[own_chunk * CORES + 1]
        query_pos = own_chunk * rows + lax.broadcasted_iota(jnp.int32, (span, rows), 1)

        def one_block(block, state):
            first = pl.multiple_of(block * span, span)
            keys = k_ref[pl.ds(first, span), :]
            values = v_ref[pl.ds(first, span), :]
            key_docs = []
            for piece in range(chunk):
                at = (block * chunk + piece) * CORES
                key_docs.append(jnp.broadcast_to(d_ref[at] + d_ref[at + 1], (rows, rows)).T)
            key_docs = jnp.concatenate(key_docs, axis=0)
            key_pos = first + lax.broadcasted_iota(jnp.int32, (span, rows), 0)
            allowed = (key_docs == own_docs) & (key_pos <= query_pos)
            bias = jnp.where(allowed, 0.0, NEG_FILL)
            bias = jnp.concatenate([bias, bias], axis=1)
            peaks, totals = [], []
            for pair in range(pairs):
                queries = jnp.concatenate(
                    [
                        q_ref[strip, core, :, h * HEAD_SIZE:(h + 1) * HEAD_SIZE]
                        for h in (2 * pair, 2 * pair + 1)
                        for core in range(CORES)
                    ],
                    axis=0,
                )
                scores = lax.dot_general(
                    keys, queries, (((1,), (1,)), ((), ())), preferred_element_type=jnp.float32
                )
                scores = jnp.where(bias < 0.0, NEG_FILL, scores)
                peak = jnp.maximum(state[0][pair], jnp.max(scores, axis=0, keepdims=True))
                weights = jnp.exp2((scores - peak) * SCALE_LOG2)
                factor = jnp.exp2((state[0][pair] - peak) * SCALE_LOG2)
                peaks.append(peak)
                totals.append(
                    state[1][pair] * factor + jnp.sum(weights, axis=0, keepdims=True)
                )
                acc[pair] = acc[pair] * factor + lax.dot_general(
                    values, weights.astype(jnp.bfloat16), (((0,), (0,)), ((), ())),
                    preferred_element_type=jnp.float32,
                )
            return tuple(peaks), tuple(totals)

        start = (
            tuple(jnp.full((1, 2 * rows), NEG_FILL, jnp.float32) for _ in range(pairs)),
            tuple(jnp.zeros((1, 2 * rows), jnp.float32) for _ in range(pairs)),
        )
        _, totals = lax.fori_loop(low, high, one_block, start)
        for pair in range(pairs):
            result = acc[pair] / totals[pair]
            for half in range(2):
                head = 2 * pair + half
                turned = result[:, half * rows:(half + 1) * rows].T.astype(jnp.bfloat16)
                for core in range(CORES):
                    o_ref[strip, core, :, head * HEAD_SIZE:(head + 1) * HEAD_SIZE] = turned[
                        core * tokens:(core + 1) * tokens
                    ]
        return carry

    lax.fori_loop(0, strips, one_strip, 0)


def return_kernel(slots, a_ref, o_ref, send, recv, own):
    kv_here, level, core = place()
    me = kv_here * CORES + core
    width = a_ref.shape[3]
    barrier = pltpu.get_barrier_semaphore()
    for step in range(1, slots):
        peer = lax.rem(me + step, slots)
        pl.semaphore_signal(barrier, inc=1, device_id=peer_id(peer, level), device_id_type=MESH)

    def target(slot):
        return o_ref.at[:, pl.ds(pl.multiple_of(slot * width, HEAD_SIZE), width)]

    local = pltpu.make_async_copy(a_ref.at[kv_here, core], target(me), own)
    local.start()
    pl.semaphore_wait(barrier, slots - 1)

    def copy(step):
        peer = lax.rem(me + step, slots)
        return pltpu.make_async_remote_copy(
            src_ref=a_ref.at[peer // CORES, lax.rem(peer, CORES)], dst_ref=target(me),
            send_sem=send.at[peer], recv_sem=recv.at[me],
            device_id=peer_id(peer, level), device_id_type=MESH,
        )

    for step in range(1, slots):
        copy(step).start()
    for step in range(1, slots):
        source = lax.rem(me + step, slots)
        pltpu.make_async_remote_copy(
            src_ref=target(source), dst_ref=target(source),
            send_sem=send.at[source], recv_sem=recv.at[source],
            device_id=peer_id(source, level), device_id_type=MESH,
        ).wait_recv()
    for step in range(1, slots):
        copy(step).wait_send()
    local.wait()


def local(strips, levels, queries, key_rows, value_matrix, doc_ids):
    slots = strips * CORES
    tokens, columns = queries.shape
    width = columns // slots
    heads = width // HEAD_SIZE
    sequence = tokens * slots * levels
    core = lax.rem(lax.axis_index("head"), CORES)
    doc_row = jnp.stack([doc_ids, doc_ids])
    doc_row = jnp.where(jnp.arange(CORES)[:, None] == core, doc_row, 0)
    doc_row = doc_row.reshape(1, CORES * tokens)
    vmem = pl.BlockSpec(memory_space=pltpu.VMEM)
    anywhere = pl.BlockSpec(memory_space=pl.ANY)
    bf16 = jnp.bfloat16
    dma = pltpu.SemaphoreType.DMA
    query_block, key_block, value_block, docs = pl.pallas_call(
        functools.partial(gather_kernel, slots, levels),
        name="gather",
        out_shape=(
            jax.ShapeDtypeStruct((strips, CORES, tokens, width), bf16),
            jax.ShapeDtypeStruct((strips, levels, CORES, tokens, HEAD_SIZE), bf16),
            jax.ShapeDtypeStruct((strips, levels, CORES, tokens, HEAD_SIZE), bf16),
            jax.ShapeDtypeStruct((strips, levels, CORES, 1, CORES * tokens), jnp.int32),
        ),
        in_specs=[anywhere, anywhere, anywhere, vmem],
        out_specs=(vmem, vmem, vmem, vmem),
        scratch_shapes=[(
            dma((4, slots)), dma((4, slots)),
            dma((3, strips, levels, 2)), dma((3, strips, levels)), dma((4,)),
        )],
        compiler_params=pltpu.CompilerParams(collective_id=0, has_side_effects=True),
    )(queries, key_rows, value_matrix, doc_row)
    docs = docs.reshape(sequence // tokens, 1, CORES * tokens)
    span = 2 * CORES * tokens
    attended = pl.pallas_call(
        functools.partial(attend_kernel, levels, heads, tokens, span),
        name="attend",
        out_shape=jax.ShapeDtypeStruct((strips, CORES, tokens, width), bf16),
        in_specs=[pl.BlockSpec(memory_space=pltpu.SMEM), vmem, vmem, vmem, vmem],
        out_specs=vmem,
        scratch_shapes=[
            pltpu.VMEM((heads // 2, HEAD_SIZE, 2 * CORES * tokens), jnp.float32),
        ],
    )(
        docs.reshape(sequence // tokens, CORES * tokens),
        query_block,
        key_block.reshape(sequence, HEAD_SIZE),
        value_block.reshape(sequence, HEAD_SIZE),
        docs,
    )
    return pl.pallas_call(
        functools.partial(return_kernel, slots),
        name="give_back",
        out_shape=jax.ShapeDtypeStruct((tokens, columns), bf16),
        in_specs=[vmem],
        out_specs=anywhere,
        scratch_shapes=[dma((slots,)), dma((slots,)), dma],
        compiler_params=pltpu.CompilerParams(collective_id=1, has_side_effects=True),
    )(attended)


def solution(mesh):
    rows = P(("kv", "head"), None)
    return jax.shard_map(
        functools.partial(local, mesh.shape["kv"], mesh.shape["head"] // CORES),
        mesh=mesh,
        in_specs=(rows, rows, rows, P(("kv", "head"))),
        out_specs=rows,
        check_vma=False,
    )
```

```python
import functools
import math

import jax
import jax.numpy as jnp
from jax import lax
from jax.experimental import pallas as pl
from jax.experimental.pallas import tpu as pltpu
from jax.sharding import PartitionSpec as P

QUERY_HEADS = 64
KEY_VALUE_HEADS = 8
HEAD_SIZE = 128
CORES = 2
NEG_FILL = -1e30
SCALE_LOG2 = HEAD_SIZE ** -0.5 * math.log2(math.e)
MESH = pl.DeviceIdType.MESH


def peer_id(slot, level):
    return {"kv": slot // CORES, "head": level * CORES + slot % CORES}


def order(slots):
    return sorted(range(1, slots), key=lambda step: (bin(step // CORES).count("1"), step))


def place():
    kv_here, head_here = lax.axis_index("kv"), lax.axis_index("head")
    return kv_here, head_here // CORES, lax.rem(head_here, CORES)


def gather_kernel(slots, levels, q_ref, k_ref, v_ref, d_ref, qo, ko, vo, do, sems):
    kv_here, level, core = place()
    me = kv_here * CORES + core
    width = q_ref.shape[1] // slots
    query_heads = width // HEAD_SIZE
    group = QUERY_HEADS // KEY_VALUE_HEADS
    slab_send, slab_recv, line_send, line_recv, own = sems

    barrier = pltpu.get_barrier_semaphore()
    for step in range(1, slots):
        peer = lax.rem(me + step, slots)
        pl.semaphore_signal(barrier, inc=1, device_id=peer_id(peer, level), device_id_type=MESH)

    @pl.when(level > 0)
    def _():
        pl.semaphore_signal(barrier, inc=1, device_id=peer_id(me, level - 1), device_id_type=MESH)

    @pl.when(level < levels - 1)
    def _():
        pl.semaphore_signal(barrier, inc=1, device_id=peer_id(me, level + 1), device_id_type=MESH)

    def parts(slot):
        kv_column = pl.multiple_of((slot * query_heads // group) * HEAD_SIZE, HEAD_SIZE)
        q_column = pl.multiple_of(slot * width, HEAD_SIZE)
        return (
            (k_ref.at[:, pl.ds(kv_column, HEAD_SIZE)], ko.at[kv_here, level, core]),
            (v_ref.at[:, pl.ds(kv_column, HEAD_SIZE)], vo.at[kv_here, level, core]),
            (d_ref, do.at[kv_here, level, core]),
            (q_ref.at[:, pl.ds(q_column, width)], qo.at[kv_here, core]),
        )

    local = [pltpu.make_async_copy(s, d, own.at[i]) for i, (s, d) in enumerate(parts(me))]
    for copy in local:
        copy.start()
    pl.semaphore_wait(
        barrier,
        slots - 1 + (level > 0).astype(jnp.int32) + (level < levels - 1).astype(jnp.int32),
    )

    def slab_copy(step, part):
        peer = me ^ step
        source, target = parts(peer)[part]
        return pltpu.make_async_remote_copy(
            src_ref=source, dst_ref=target,
            send_sem=slab_send.at[part, peer], recv_sem=slab_recv.at[part, me],
            device_id=peer_id(peer, level), device_id_type=MESH,
        )

    for part in range(4):
        for step in order(slots):
            slab_copy(step, part).start()

    def slab_wait(part, source):
        target = (
            ko.at[source // CORES, level, lax.rem(source, CORES)],
            vo.at[source // CORES, level, lax.rem(source, CORES)],
            do.at[source // CORES, level, lax.rem(source, CORES)],
            qo.at[source // CORES, lax.rem(source, CORES)],
        )[part]
        pltpu.make_async_remote_copy(
            src_ref=target, dst_ref=target,
            send_sem=slab_send.at[part, source], recv_sem=slab_recv.at[part, source],
            device_id=peer_id(source, level), device_id_type=MESH,
        ).wait_recv()

    buffers = (ko, vo, do)

    def line_copy(part, strip, slab, up):
        ref = buffers[part].at[strip, slab]
        return pltpu.make_async_remote_copy(
            src_ref=ref, dst_ref=ref,
            send_sem=line_send.at[part, strip, slab, 1 if up else 0],
            recv_sem=line_recv.at[part, strip, slab],
            device_id=peer_id(me, level + 1 if up else level - 1), device_id_type=MESH,
        )

    for copy in local:
        copy.wait()
    strips = slots // CORES

    def line_send_all(strip, slab, up, act):
        for part in range(3):
            copy = line_copy(part, strip, slab, up)
            copy.start() if act else copy.wait_send()

    for ahead in range(strips):
        strip = lax.rem(kv_here + ahead, strips)
        for source_core in range(CORES):
            source = strip * CORES + source_core

            @pl.when(source != me)
            def _():
                for part in range(3):
                    slab_wait(part, source)

        @pl.when(level < levels - 1)
        def _():
            line_send_all(strip, level, True, True)

        @pl.when(level > 0)
        def _():
            line_send_all(strip, level, False, True)

    for step in range(1, levels):
        for ahead in range(strips):
            strip = lax.rem(kv_here + ahead, strips)
            for up in (True, False):
                slab = level - step if up else level + step
                exists = (slab >= 0) if up else (slab < levels)
                onward = (level < levels - 1) if up else (level > 0)

                @pl.when(exists)
                def _():
                    for part in range(3):
                        line_copy(part, strip, slab, True).wait_recv()

                @pl.when(exists & onward)
                def _():
                    line_send_all(strip, slab, up, True)

    for step in range(0, levels):
        for strip in range(strips):
            for up in (True, False):
                slab = level - step if up else level + step
                exists = (slab >= 0) if up else (slab < levels)
                onward = (level < levels - 1) if up else (level > 0)

                @pl.when(exists & onward)
                def _():
                    line_send_all(strip, slab, up, False)

    for step in range(1, slots):
        slab_wait(3, lax.rem(me + step, slots))
    for part in range(4):
        for step in range(1, slots):
            slab_copy(step, part).wait_send()


def attend_kernel(levels, heads, tokens, span, docs_ref, q_ref, k_ref, v_ref, d_ref, o_ref, acc):
    strips = q_ref.shape[0]
    rows = CORES * tokens
    level = lax.axis_index("head") // CORES
    pairs = heads // 2
    chunk = span // rows
    blocks = k_ref.shape[0] // span

    def one_strip(strip, carry):
        own_chunk = strip * levels + level
        first_doc = docs_ref[own_chunk * CORES, 0]
        high = own_chunk // chunk + 1

        def count(block, low):
            last = docs_ref[(block + 1) * chunk * CORES - 1, rows - 1]
            return low + jnp.where(last < first_doc, 1, 0)

        low = lax.fori_loop(0, high - 1, count, 0)
        acc[...] = jnp.zeros_like(acc)
        own_docs = d_ref[own_chunk * CORES] + d_ref[own_chunk * CORES + 1]
        query_pos = own_chunk * rows + lax.broadcasted_iota(jnp.int32, (span, rows), 1)

        def one_block(block, state):
            first = pl.multiple_of(block * span, span)
            keys = k_ref[pl.ds(first, span), :]
            values = v_ref[pl.ds(first, span), :].T
            key_docs = []
            for piece in range(chunk):
                at = (block * chunk + piece) * CORES
                key_docs.append(jnp.broadcast_to(d_ref[at] + d_ref[at + 1], (rows, rows)).T)
            key_docs = jnp.concatenate(key_docs, axis=0)
            key_pos = first + lax.broadcasted_iota(jnp.int32, (span, rows), 0)
            allowed = (key_docs == own_docs) & (key_pos <= query_pos)
            bias = jnp.where(allowed, 0.0, NEG_FILL)
            bias = jnp.concatenate([bias, bias], axis=1)
            peaks, totals = [], []
            for pair in range(pairs):
                queries = jnp.concatenate(
                    [
                        q_ref[strip, core, :, h * HEAD_SIZE:(h + 1) * HEAD_SIZE]
                        for h in (2 * pair, 2 * pair + 1)
                        for core in range(CORES)
                    ],
                    axis=0,
                )
                scores = lax.dot_general(
                    keys, queries, (((1,), (1,)), ((), ())), preferred_element_type=jnp.float32
                )
                scores = scores + bias
                peak = jnp.maximum(state[0][pair], jnp.max(scores, axis=0, keepdims=True))
                weights = jnp.exp2((scores - peak) * SCALE_LOG2)
                factor = jnp.exp2((state[0][pair] - peak) * SCALE_LOG2)
                peaks.append(peak)
                totals.append(
                    state[1][pair] * factor + jnp.sum(weights, axis=0, keepdims=True)
                )
                acc[pair] = acc[pair] * factor + lax.dot_general(
                    values, weights.astype(jnp.bfloat16), (((1,), (0,)), ((), ())),
                    preferred_element_type=jnp.float32,
                )
            return tuple(peaks), tuple(totals)

        start = (
            tuple(jnp.full((1, 2 * rows), NEG_FILL, jnp.float32) for _ in range(pairs)),
            tuple(jnp.zeros((1, 2 * rows), jnp.float32) for _ in range(pairs)),
        )
        _, totals = lax.fori_loop(low, high, one_block, start)
        for pair in range(pairs):
            result = acc[pair] / totals[pair]
            for half in range(2):
                head = 2 * pair + half
                turned = result[:, half * rows:(half + 1) * rows].T.astype(jnp.bfloat16)
                for core in range(CORES):
                    o_ref[strip, core, :, head * HEAD_SIZE:(head + 1) * HEAD_SIZE] = turned[
                        core * tokens:(core + 1) * tokens
                    ]
        return carry

    lax.fori_loop(0, strips, one_strip, 0)


def return_kernel(slots, a_ref, o_ref, send, recv, own):
    kv_here, level, core = place()
    me = kv_here * CORES + core
    width = a_ref.shape[3]
    barrier = pltpu.get_barrier_semaphore()
    for step in range(1, slots):
        peer = lax.rem(me + step, slots)
        pl.semaphore_signal(barrier, inc=1, device_id=peer_id(peer, level), device_id_type=MESH)

    def target(slot):
        return o_ref.at[:, pl.ds(pl.multiple_of(slot * width, HEAD_SIZE), width)]

    local = pltpu.make_async_copy(a_ref.at[kv_here, core], target(me), own)
    local.start()
    pl.semaphore_wait(barrier, slots - 1)

    def copy(step):
        peer = me ^ step
        return pltpu.make_async_remote_copy(
            src_ref=a_ref.at[peer // CORES, lax.rem(peer, CORES)], dst_ref=target(me),
            send_sem=send.at[peer], recv_sem=recv.at[me],
            device_id=peer_id(peer, level), device_id_type=MESH,
        )

    for step in order(slots):
        copy(step).start()
    for step in range(1, slots):
        source = lax.rem(me + step, slots)
        pltpu.make_async_remote_copy(
            src_ref=target(source), dst_ref=target(source),
            send_sem=send.at[source], recv_sem=recv.at[source],
            device_id=peer_id(source, level), device_id_type=MESH,
        ).wait_recv()
    for step in range(1, slots):
        copy(step).wait_send()
    local.wait()


def local(strips, levels, queries, key_rows, value_matrix, doc_ids):
    slots = strips * CORES
    tokens, columns = queries.shape
    width = columns // slots
    heads = width // HEAD_SIZE
    sequence = tokens * slots * levels
    core = lax.rem(lax.axis_index("head"), CORES)
    doc_row = jnp.stack([doc_ids, doc_ids])
    doc_row = jnp.where(jnp.arange(CORES)[:, None] == core, doc_row, 0)
    doc_row = doc_row.reshape(1, CORES * tokens)
    vmem = pl.BlockSpec(memory_space=pltpu.VMEM)
    anywhere = pl.BlockSpec(memory_space=pl.ANY)
    bf16 = jnp.bfloat16
    dma = pltpu.SemaphoreType.DMA
    query_block, key_block, value_block, docs = pl.pallas_call(
        functools.partial(gather_kernel, slots, levels),
        name="gather",
        out_shape=(
            jax.ShapeDtypeStruct((strips, CORES, tokens, width), bf16),
            jax.ShapeDtypeStruct((strips, levels, CORES, tokens, HEAD_SIZE), bf16),
            jax.ShapeDtypeStruct((strips, levels, CORES, tokens, HEAD_SIZE), bf16),
            jax.ShapeDtypeStruct((strips, levels, CORES, 1, CORES * tokens), jnp.int32),
        ),
        in_specs=[anywhere, anywhere, anywhere, vmem],
        out_specs=(vmem, vmem, vmem, vmem),
        scratch_shapes=[(
            dma((4, slots)), dma((4, slots)),
            dma((3, strips, levels, 2)), dma((3, strips, levels)), dma((4,)),
        )],
        compiler_params=pltpu.CompilerParams(collective_id=0, has_side_effects=True),
    )(queries, key_rows, value_matrix, doc_row)
    docs = docs.reshape(sequence // tokens, 1, CORES * tokens)
    span = 2 * CORES * tokens
    attended = pl.pallas_call(
        functools.partial(attend_kernel, levels, heads, tokens, span),
        name="attend",
        out_shape=jax.ShapeDtypeStruct((strips, CORES, tokens, width), bf16),
        in_specs=[pl.BlockSpec(memory_space=pltpu.SMEM), vmem, vmem, vmem, vmem],
        out_specs=vmem,
        scratch_shapes=[
            pltpu.VMEM((heads // 2, HEAD_SIZE, 2 * CORES * tokens), jnp.float32),
        ],
    )(
        docs.reshape(sequence // tokens, CORES * tokens),
        query_block,
        key_block.reshape(sequence, HEAD_SIZE),
        value_block.reshape(sequence, HEAD_SIZE),
        docs,
    )
    return pl.pallas_call(
        functools.partial(return_kernel, slots),
        name="give_back",
        out_shape=jax.ShapeDtypeStruct((tokens, columns), bf16),
        in_specs=[vmem],
        out_specs=anywhere,
        scratch_shapes=[dma((slots,)), dma((slots,)), dma],
        compiler_params=pltpu.CompilerParams(collective_id=1, has_side_effects=True),
    )(attended)


def solution(mesh):
    rows = P(("kv", "head"), None)
    return jax.shard_map(
        functools.partial(local, mesh.shape["kv"], mesh.shape["head"] // CORES),
        mesh=mesh,
        in_specs=(rows, rows, rows, P(("kv", "head"))),
        out_specs=rows,
        check_vma=False,
    )
```

```python
import functools
import math

import jax
import jax.numpy as jnp
from jax import lax
from jax.experimental import pallas as pl
from jax.experimental.pallas import tpu as pltpu
from jax.sharding import PartitionSpec as P

QUERY_HEADS = 64
KEY_VALUE_HEADS = 8
HEAD_SIZE = 128
CORES = 2
NEG_FILL = -1e30
SCALE_LOG2 = HEAD_SIZE ** -0.5 * math.log2(math.e)
MESH = pl.DeviceIdType.MESH


def peer_id(slot, level):
    return {"kv": slot // CORES, "head": level * CORES + slot % CORES}


def order(slots):
    return sorted(range(1, slots), key=lambda step: (bin(step // CORES).count("1"), step))


def place():
    kv_here, head_here = lax.axis_index("kv"), lax.axis_index("head")
    return kv_here, head_here // CORES, lax.rem(head_here, CORES)


def gather_kernel(slots, levels, q_ref, k_ref, v_ref, d_ref, qo, ko, vo, do, sems):
    kv_here, level, core = place()
    me = kv_here * CORES + core
    width = q_ref.shape[1] // slots
    query_heads = width // HEAD_SIZE
    group = QUERY_HEADS // KEY_VALUE_HEADS
    slab_send, slab_recv, line_send, line_recv, own = sems

    barrier = pltpu.get_barrier_semaphore()
    for step in range(1, slots):
        peer = lax.rem(me + step, slots)
        pl.semaphore_signal(barrier, inc=1, device_id=peer_id(peer, level), device_id_type=MESH)

    @pl.when(level > 0)
    def _():
        pl.semaphore_signal(barrier, inc=1, device_id=peer_id(me, level - 1), device_id_type=MESH)

    @pl.when(level < levels - 1)
    def _():
        pl.semaphore_signal(barrier, inc=1, device_id=peer_id(me, level + 1), device_id_type=MESH)

    def parts(slot):
        kv_column = pl.multiple_of((slot * query_heads // group) * HEAD_SIZE, HEAD_SIZE)
        q_column = pl.multiple_of(slot * width, HEAD_SIZE)
        return (
            (k_ref.at[:, pl.ds(kv_column, HEAD_SIZE)], ko.at[kv_here, level, core]),
            (v_ref.at[:, pl.ds(kv_column, HEAD_SIZE)], vo.at[kv_here, level, core]),
            (d_ref, do.at[kv_here, level, core]),
            (q_ref.at[:, pl.ds(q_column, width)], qo.at[kv_here, core]),
        )

    local = [pltpu.make_async_copy(s, d, own.at[i]) for i, (s, d) in enumerate(parts(me))]
    for copy in local:
        copy.start()
    pl.semaphore_wait(
        barrier,
        slots - 1 + (level > 0).astype(jnp.int32) + (level < levels - 1).astype(jnp.int32),
    )

    def slab_copy(step, part):
        peer = me ^ step
        source, target = parts(peer)[part]
        return pltpu.make_async_remote_copy(
            src_ref=source, dst_ref=target,
            send_sem=slab_send.at[part, peer], recv_sem=slab_recv.at[part, me],
            device_id=peer_id(peer, level), device_id_type=MESH,
        )

    for part in range(4):
        for step in order(slots):
            slab_copy(step, part).start()

    def slab_wait(part, source):
        target = (
            ko.at[source // CORES, level, lax.rem(source, CORES)],
            vo.at[source // CORES, level, lax.rem(source, CORES)],
            do.at[source // CORES, level, lax.rem(source, CORES)],
            qo.at[source // CORES, lax.rem(source, CORES)],
        )[part]
        pltpu.make_async_remote_copy(
            src_ref=target, dst_ref=target,
            send_sem=slab_send.at[part, source], recv_sem=slab_recv.at[part, source],
            device_id=peer_id(source, level), device_id_type=MESH,
        ).wait_recv()

    buffers = (ko, vo, do)

    def line_copy(part, strip, slab, up):
        ref = buffers[part].at[strip, slab]
        return pltpu.make_async_remote_copy(
            src_ref=ref, dst_ref=ref,
            send_sem=line_send.at[part, strip, slab, 1 if up else 0],
            recv_sem=line_recv.at[part, strip, slab],
            device_id=peer_id(me, level + 1 if up else level - 1), device_id_type=MESH,
        )

    for copy in local:
        copy.wait()
    strips = slots // CORES

    def line_send_all(strip, slab, up, act):
        for part in range(3):
            copy = line_copy(part, strip, slab, up)
            copy.start() if act else copy.wait_send()

    for ahead in range(strips):
        strip = lax.rem(kv_here + ahead, strips)
        for source_core in range(CORES):
            source = strip * CORES + source_core

            @pl.when(source != me)
            def _():
                for part in range(3):
                    slab_wait(part, source)

        @pl.when(level < levels - 1)
        def _():
            line_send_all(strip, level, True, True)

        @pl.when(level > 0)
        def _():
            line_send_all(strip, level, False, True)

    for step in range(1, levels):
        for ahead in range(strips):
            strip = lax.rem(kv_here + ahead, strips)
            for up in (True, False):
                slab = level - step if up else level + step
                exists = (slab >= 0) if up else (slab < levels)
                onward = (level < levels - 1) if up else (level > 0)

                @pl.when(exists)
                def _():
                    for part in range(3):
                        line_copy(part, strip, slab, True).wait_recv()

                @pl.when(exists & onward)
                def _():
                    line_send_all(strip, slab, up, True)

    for step in range(0, levels):
        for strip in range(strips):
            for up in (True, False):
                slab = level - step if up else level + step
                exists = (slab >= 0) if up else (slab < levels)
                onward = (level < levels - 1) if up else (level > 0)

                @pl.when(exists & onward)
                def _():
                    line_send_all(strip, slab, up, False)

    for step in range(1, slots):
        slab_wait(3, lax.rem(me + step, slots))
    for part in range(4):
        for step in range(1, slots):
            slab_copy(step, part).wait_send()


def attend_kernel(levels, heads, tokens, span, docs_ref, q_ref, k_ref, v_ref, d_ref, o_ref, acc, held, rounded):
    strips = q_ref.shape[0]
    rows = CORES * tokens
    level = lax.axis_index("head") // CORES
    pairs = heads // 2
    chunk = span // rows
    blocks = k_ref.shape[0] // span

    def one_strip(strip, carry):
        own_chunk = strip * levels + level
        first_doc = docs_ref[own_chunk * CORES, 0]
        high = own_chunk // chunk + 1

        def count(block, low):
            last = docs_ref[(block + 1) * chunk * CORES - 1, rows - 1]
            return low + jnp.where(last < first_doc, 1, 0)

        low = lax.fori_loop(0, high - 1, count, 0)
        acc[...] = jnp.zeros_like(acc)
        own_docs = d_ref[own_chunk * CORES] + d_ref[own_chunk * CORES + 1]
        query_pos = own_chunk * rows + lax.broadcasted_iota(jnp.int32, (span, rows), 1)

        def one_block(block, state):
            first = pl.multiple_of(block * span, span)
            keys = k_ref[pl.ds(first, span), :]
            values = v_ref[pl.ds(first, span), :].T
            key_docs = []
            for piece in range(chunk):
                at = (block * chunk + piece) * CORES
                key_docs.append(jnp.broadcast_to(d_ref[at] + d_ref[at + 1], (rows, rows)).T)
            key_docs = jnp.concatenate(key_docs, axis=0)
            key_pos = first + lax.broadcasted_iota(jnp.int32, (span, rows), 0)
            allowed = (key_docs == own_docs) & (key_pos <= query_pos)
            bias = jnp.where(allowed, 0.0, NEG_FILL)
            bias = jnp.concatenate([bias, bias], axis=1)
            peaks, totals = [], []

            def score(pair):
                queries = jnp.concatenate(
                    [
                        q_ref[strip, core, :, h * HEAD_SIZE:(h + 1) * HEAD_SIZE]
                        for h in (2 * pair, 2 * pair + 1)
                        for core in range(CORES)
                    ],
                    axis=0,
                )
                scores = lax.dot_general(
                    keys, queries, (((1,), (1,)), ((), ())), preferred_element_type=jnp.float32
                ) + bias
                held[pair] = scores
                peaks.append(
                    jnp.maximum(state[0][pair], jnp.max(scores, axis=0, keepdims=True))
                )

            def weigh(pair):
                peak = peaks[pair]
                weights = jnp.exp2((held[pair] - peak) * SCALE_LOG2)
                factor = jnp.exp2((state[0][pair] - peak) * SCALE_LOG2)
                totals.append(
                    state[1][pair] * factor + jnp.sum(weights, axis=0, keepdims=True)
                )
                rounded[pair] = weights.astype(jnp.bfloat16)
                factors.append(factor)

            def fold(pair):
                acc[pair] = acc[pair] * factors[pair] + lax.dot_general(
                    values, rounded[pair], (((1,), (0,)), ((), ())),
                    preferred_element_type=jnp.float32,
                )

            factors = []
            score(0)
            for pair in range(pairs):
                if pair + 1 < pairs:
                    score(pair + 1)
                weigh(pair)
                if pair >= 1:
                    fold(pair - 1)
            fold(pairs - 1)
            return tuple(peaks), tuple(totals)

        start = (
            tuple(jnp.full((1, 2 * rows), NEG_FILL, jnp.float32) for _ in range(pairs)),
            tuple(jnp.zeros((1, 2 * rows), jnp.float32) for _ in range(pairs)),
        )
        _, totals = lax.fori_loop(low, high, one_block, start)
        for pair in range(pairs):
            result = acc[pair] / totals[pair]
            for half in range(2):
                head = 2 * pair + half
                turned = result[:, half * rows:(half + 1) * rows].T.astype(jnp.bfloat16)
                for core in range(CORES):
                    o_ref[strip, core, :, head * HEAD_SIZE:(head + 1) * HEAD_SIZE] = turned[
                        core * tokens:(core + 1) * tokens
                    ]
        return carry

    lax.fori_loop(0, strips, one_strip, 0)


def return_kernel(slots, a_ref, o_ref, send, recv, own):
    kv_here, level, core = place()
    me = kv_here * CORES + core
    width = a_ref.shape[3]
    barrier = pltpu.get_barrier_semaphore()
    for step in range(1, slots):
        peer = lax.rem(me + step, slots)
        pl.semaphore_signal(barrier, inc=1, device_id=peer_id(peer, level), device_id_type=MESH)

    def target(slot):
        return o_ref.at[:, pl.ds(pl.multiple_of(slot * width, HEAD_SIZE), width)]

    local = pltpu.make_async_copy(a_ref.at[kv_here, core], target(me), own)
    local.start()
    pl.semaphore_wait(barrier, slots - 1)

    def copy(step):
        peer = me ^ step
        return pltpu.make_async_remote_copy(
            src_ref=a_ref.at[peer // CORES, lax.rem(peer, CORES)], dst_ref=target(me),
            send_sem=send.at[peer], recv_sem=recv.at[me],
            device_id=peer_id(peer, level), device_id_type=MESH,
        )

    for step in order(slots):
        copy(step).start()
    for step in range(1, slots):
        source = lax.rem(me + step, slots)
        pltpu.make_async_remote_copy(
            src_ref=target(source), dst_ref=target(source),
            send_sem=send.at[source], recv_sem=recv.at[source],
            device_id=peer_id(source, level), device_id_type=MESH,
        ).wait_recv()
    for step in range(1, slots):
        copy(step).wait_send()
    local.wait()


def local(strips, levels, queries, key_rows, value_matrix, doc_ids):
    slots = strips * CORES
    tokens, columns = queries.shape
    width = columns // slots
    heads = width // HEAD_SIZE
    sequence = tokens * slots * levels
    core = lax.rem(lax.axis_index("head"), CORES)
    doc_row = jnp.stack([doc_ids, doc_ids])
    doc_row = jnp.where(jnp.arange(CORES)[:, None] == core, doc_row, 0)
    doc_row = doc_row.reshape(1, CORES * tokens)
    vmem = pl.BlockSpec(memory_space=pltpu.VMEM)
    anywhere = pl.BlockSpec(memory_space=pl.ANY)
    bf16 = jnp.bfloat16
    dma = pltpu.SemaphoreType.DMA
    query_block, key_block, value_block, docs = pl.pallas_call(
        functools.partial(gather_kernel, slots, levels),
        name="gather",
        out_shape=(
            jax.ShapeDtypeStruct((strips, CORES, tokens, width), bf16),
            jax.ShapeDtypeStruct((strips, levels, CORES, tokens, HEAD_SIZE), bf16),
            jax.ShapeDtypeStruct((strips, levels, CORES, tokens, HEAD_SIZE), bf16),
            jax.ShapeDtypeStruct((strips, levels, CORES, 1, CORES * tokens), jnp.int32),
        ),
        in_specs=[anywhere, anywhere, anywhere, vmem],
        out_specs=(vmem, vmem, vmem, vmem),
        scratch_shapes=[(
            dma((4, slots)), dma((4, slots)),
            dma((3, strips, levels, 2)), dma((3, strips, levels)), dma((4,)),
        )],
        compiler_params=pltpu.CompilerParams(collective_id=0, has_side_effects=True),
    )(queries, key_rows, value_matrix, doc_row)
    docs = docs.reshape(sequence // tokens, 1, CORES * tokens)
    span = 2 * CORES * tokens
    attended = pl.pallas_call(
        functools.partial(attend_kernel, levels, heads, tokens, span),
        name="attend",
        out_shape=jax.ShapeDtypeStruct((strips, CORES, tokens, width), bf16),
        in_specs=[pl.BlockSpec(memory_space=pltpu.SMEM), vmem, vmem, vmem, vmem],
        out_specs=vmem,
        scratch_shapes=[
            pltpu.VMEM((heads // 2, HEAD_SIZE, 2 * CORES * tokens), jnp.float32),
            pltpu.VMEM((heads // 2, span, 2 * CORES * tokens), jnp.float32),
            pltpu.VMEM((heads // 2, span, 2 * CORES * tokens), bf16),
        ],
    )(
        docs.reshape(sequence // tokens, CORES * tokens),
        query_block,
        key_block.reshape(sequence, HEAD_SIZE),
        value_block.reshape(sequence, HEAD_SIZE),
        docs,
    )
    return pl.pallas_call(
        functools.partial(return_kernel, slots),
        name="give_back",
        out_shape=jax.ShapeDtypeStruct((tokens, columns), bf16),
        in_specs=[vmem],
        out_specs=anywhere,
        scratch_shapes=[dma((slots,)), dma((slots,)), dma],
        compiler_params=pltpu.CompilerParams(collective_id=1, has_side_effects=True),
    )(attended)


def solution(mesh):
    rows = P(("kv", "head"), None)
    return jax.shard_map(
        functools.partial(local, mesh.shape["kv"], mesh.shape["head"] // CORES),
        mesh=mesh,
        in_specs=(rows, rows, rows, P(("kv", "head"))),
        out_specs=rows,
        check_vma=False,
    )
```

```python
import functools
import math

import jax
import jax.numpy as jnp
from jax import lax
from jax.experimental import pallas as pl
from jax.experimental.pallas import tpu as pltpu
from jax.sharding import PartitionSpec as P

QUERY_HEADS = 64
KEY_VALUE_HEADS = 8
HEAD_SIZE = 128
CORES = 2
NEG_FILL = -1e30
SCALE_LOG2 = HEAD_SIZE ** -0.5 * math.log2(math.e)
MESH = pl.DeviceIdType.MESH


def peer_id(slot, level):
    return {"kv": slot // CORES, "head": level * CORES + slot % CORES}


def order(slots):
    return sorted(range(1, slots), key=lambda step: (bin(step // CORES).count("1"), step))


def place():
    kv_here, head_here = lax.axis_index("kv"), lax.axis_index("head")
    return kv_here, head_here // CORES, lax.rem(head_here, CORES)


def gather_kernel(slots, levels, q_ref, k_ref, v_ref, d_ref, qo, kvo, do, sems):
    kv_here, level, core = place()
    me = kv_here * CORES + core
    width = q_ref.shape[1] // slots
    query_heads = width // HEAD_SIZE
    group = QUERY_HEADS // KEY_VALUE_HEADS
    slab_send, slab_recv, line_send, line_recv, own = sems

    barrier = pltpu.get_barrier_semaphore()
    for step in range(1, slots):
        peer = lax.rem(me + step, slots)
        pl.semaphore_signal(barrier, inc=1, device_id=peer_id(peer, level), device_id_type=MESH)

    @pl.when(level > 0)
    def _():
        pl.semaphore_signal(barrier, inc=1, device_id=peer_id(me, level - 1), device_id_type=MESH)

    @pl.when(level < levels - 1)
    def _():
        pl.semaphore_signal(barrier, inc=1, device_id=peer_id(me, level + 1), device_id_type=MESH)

    def parts(slot):
        kv_column = pl.multiple_of((slot * query_heads // group) * HEAD_SIZE, HEAD_SIZE)
        q_column = pl.multiple_of(slot * width, HEAD_SIZE)
        return (
            (k_ref.at[:, pl.ds(kv_column, HEAD_SIZE)], kvo.at[kv_here, level, core, 0]),
            (v_ref.at[:, pl.ds(kv_column, HEAD_SIZE)], kvo.at[kv_here, level, core, 1]),
            (d_ref, do.at[kv_here, level, core]),
            (q_ref.at[:, pl.ds(q_column, width)], qo.at[kv_here, core]),
        )

    local = [pltpu.make_async_copy(s, d, own.at[i]) for i, (s, d) in enumerate(parts(me))]
    for copy in local:
        copy.start()
    pl.semaphore_wait(
        barrier,
        slots - 1 + (level > 0).astype(jnp.int32) + (level < levels - 1).astype(jnp.int32),
    )

    def slab_copy(step, part):
        peer = me ^ step
        source, target = parts(peer)[part]
        return pltpu.make_async_remote_copy(
            src_ref=source, dst_ref=target,
            send_sem=slab_send.at[part, peer], recv_sem=slab_recv.at[part, me],
            device_id=peer_id(peer, level), device_id_type=MESH,
        )

    for part in range(4):
        for step in order(slots):
            slab_copy(step, part).start()

    def slab_wait(part, source):
        target = (
            kvo.at[source // CORES, level, lax.rem(source, CORES), 0],
            kvo.at[source // CORES, level, lax.rem(source, CORES), 1],
            do.at[source // CORES, level, lax.rem(source, CORES)],
            qo.at[source // CORES, lax.rem(source, CORES)],
        )[part]
        pltpu.make_async_remote_copy(
            src_ref=target, dst_ref=target,
            send_sem=slab_send.at[part, source], recv_sem=slab_recv.at[part, source],
            device_id=peer_id(source, level), device_id_type=MESH,
        ).wait_recv()

    strips = slots // CORES

    def line_copy(item, slab, up):
        whole = isinstance(item, int) and item == strips
        ref = do.at[:, slab] if whole else kvo.at[item, slab]
        return pltpu.make_async_remote_copy(
            src_ref=ref, dst_ref=ref,
            send_sem=line_send.at[item, slab, 1 if up else 0],
            recv_sem=line_recv.at[item, slab],
            device_id=peer_id(me, level + 1 if up else level - 1), device_id_type=MESH,
        )

    for copy in local:
        copy.wait()

    def both_ways(item):
        @pl.when(level < levels - 1)
        def _():
            line_copy(item, level, True).start()

        @pl.when(level > 0)
        def _():
            line_copy(item, level, False).start()

    for ahead in range(strips):
        strip = kv_here ^ ahead
        for source_core in range(CORES):
            source = strip * CORES + source_core

            @pl.when(source != me)
            def _():
                for part in range(2):
                    slab_wait(part, source)

        both_ways(strip)
    for step in range(1, slots):
        slab_wait(2, me ^ step)
    both_ways(strips)

    def passes(step):
        for up in (True, False):
            slab = level - step if up else level + step
            exists = (slab >= 0) if up else (slab < levels)
            onward = (level < levels - 1) if up else (level > 0)
            yield up, slab, exists, exists & onward

    for step in range(1, levels):
        for ahead in range(strips + 1):
            item = kv_here ^ ahead if ahead < strips else strips
            for up, slab, exists, onward in passes(step):
                @pl.when(exists)
                def _():
                    line_copy(item, slab, True).wait_recv()

                @pl.when(onward)
                def _():
                    line_copy(item, slab, up).start()

    for step in range(levels):
        for item in range(strips + 1):
            for up, slab, exists, onward in passes(step):
                @pl.when(onward)
                def _():
                    line_copy(item, slab, up).wait_send()

    for step in range(1, slots):
        slab_wait(3, lax.rem(me + step, slots))
    for part in range(4):
        for step in range(1, slots):
            slab_copy(step, part).wait_send()


def attend_kernel(levels, heads, tokens, span, docs_ref, q_ref, kv_ref, d_ref, o_ref, acc, held, rounded):
    strips = q_ref.shape[0]
    rows = CORES * tokens
    level = lax.axis_index("head") // CORES
    pairs = heads // 2
    chunk = span // rows

    def one_strip(strip, carry):
        own_chunk = strip * levels + level
        first_doc = docs_ref[own_chunk * CORES, 0]
        high = own_chunk // chunk + 1

        def count(block, low):
            last = docs_ref[(block + 1) * chunk * CORES - 1, rows - 1]
            return low + jnp.where(last < first_doc, 1, 0)

        low = lax.fori_loop(0, high - 1, count, 0)
        acc[...] = jnp.zeros_like(acc)
        own_docs = d_ref[own_chunk * CORES] + d_ref[own_chunk * CORES + 1]
        query_pos = own_chunk * rows + lax.broadcasted_iota(jnp.int32, (span, rows), 1)

        def one_block(block, state):
            first = pl.multiple_of(block * span, span)
            pieces = pl.ds(block * chunk * CORES, chunk * CORES)
            keys = kv_ref[pieces, 0].reshape(span, HEAD_SIZE)
            values = kv_ref[pieces, 1].reshape(span, HEAD_SIZE).T
            key_docs = []
            for piece in range(chunk):
                at = (block * chunk + piece) * CORES
                key_docs.append(jnp.broadcast_to(d_ref[at] + d_ref[at + 1], (rows, rows)).T)
            key_docs = jnp.concatenate(key_docs, axis=0)
            key_pos = first + lax.broadcasted_iota(jnp.int32, (span, rows), 0)
            allowed = (key_docs == own_docs) & (key_pos <= query_pos)
            bias = jnp.where(allowed, 0.0, NEG_FILL)
            bias = jnp.concatenate([bias, bias], axis=1)
            peaks, totals = [], []

            def score(pair):
                queries = jnp.concatenate(
                    [
                        q_ref[strip, core, :, h * HEAD_SIZE:(h + 1) * HEAD_SIZE]
                        for h in (2 * pair, 2 * pair + 1)
                        for core in range(CORES)
                    ],
                    axis=0,
                )
                scores = lax.dot_general(
                    keys, queries, (((1,), (1,)), ((), ())), preferred_element_type=jnp.float32
                ) + bias
                held[pair] = scores
                peaks.append(
                    jnp.maximum(state[0][pair], jnp.max(scores, axis=0, keepdims=True))
                )

            def weigh(pair):
                peak = peaks[pair]
                weights = jnp.exp2((held[pair] - peak) * SCALE_LOG2)
                factor = jnp.exp2((state[0][pair] - peak) * SCALE_LOG2)
                totals.append(
                    state[1][pair] * factor + jnp.sum(weights, axis=0, keepdims=True)
                )
                rounded[pair] = weights.astype(jnp.bfloat16)
                factors.append(factor)

            def fold(pair):
                acc[pair] = acc[pair] * factors[pair] + lax.dot_general(
                    values, rounded[pair], (((1,), (0,)), ((), ())),
                    preferred_element_type=jnp.float32,
                )

            factors = []
            score(0)
            for pair in range(pairs):
                if pair + 1 < pairs:
                    score(pair + 1)
                weigh(pair)
                if pair >= 1:
                    fold(pair - 1)
            fold(pairs - 1)
            return tuple(peaks), tuple(totals)

        start = (
            tuple(jnp.full((1, 2 * rows), NEG_FILL, jnp.float32) for _ in range(pairs)),
            tuple(jnp.zeros((1, 2 * rows), jnp.float32) for _ in range(pairs)),
        )
        _, totals = lax.fori_loop(low, high, one_block, start)
        for pair in range(pairs):
            result = acc[pair] / totals[pair]
            for half in range(2):
                head = 2 * pair + half
                turned = result[:, half * rows:(half + 1) * rows].T.astype(jnp.bfloat16)
                for core in range(CORES):
                    o_ref[strip, core, :, head * HEAD_SIZE:(head + 1) * HEAD_SIZE] = turned[
                        core * tokens:(core + 1) * tokens
                    ]
        return carry

    lax.fori_loop(0, strips, one_strip, 0)


def return_kernel(slots, a_ref, o_ref, send, recv, own):
    kv_here, level, core = place()
    me = kv_here * CORES + core
    width = a_ref.shape[3]
    barrier = pltpu.get_barrier_semaphore()
    for step in range(1, slots):
        peer = lax.rem(me + step, slots)
        pl.semaphore_signal(barrier, inc=1, device_id=peer_id(peer, level), device_id_type=MESH)

    def target(slot):
        return o_ref.at[:, pl.ds(pl.multiple_of(slot * width, HEAD_SIZE), width)]

    local = pltpu.make_async_copy(a_ref.at[kv_here, core], target(me), own)
    local.start()
    pl.semaphore_wait(barrier, slots - 1)

    def copy(step):
        peer = me ^ step
        return pltpu.make_async_remote_copy(
            src_ref=a_ref.at[peer // CORES, lax.rem(peer, CORES)], dst_ref=target(me),
            send_sem=send.at[peer], recv_sem=recv.at[me],
            device_id=peer_id(peer, level), device_id_type=MESH,
        )

    for step in order(slots):
        copy(step).start()
    for step in range(1, slots):
        source = lax.rem(me + step, slots)
        pltpu.make_async_remote_copy(
            src_ref=target(source), dst_ref=target(source),
            send_sem=send.at[source], recv_sem=recv.at[source],
            device_id=peer_id(source, level), device_id_type=MESH,
        ).wait_recv()
    for step in range(1, slots):
        copy(step).wait_send()
    local.wait()


def local(strips, levels, queries, key_rows, value_matrix, doc_ids):
    slots = strips * CORES
    tokens, columns = queries.shape
    width = columns // slots
    heads = width // HEAD_SIZE
    sequence = tokens * slots * levels
    core = lax.rem(lax.axis_index("head"), CORES)
    doc_row = jnp.stack([doc_ids, doc_ids])
    doc_row = jnp.where(jnp.arange(CORES)[:, None] == core, doc_row, 0)
    doc_row = doc_row.reshape(1, CORES * tokens)
    vmem = pl.BlockSpec(memory_space=pltpu.VMEM)
    anywhere = pl.BlockSpec(memory_space=pl.ANY)
    bf16 = jnp.bfloat16
    dma = pltpu.SemaphoreType.DMA
    query_block, key_value, docs = pl.pallas_call(
        functools.partial(gather_kernel, slots, levels),
        name="gather",
        out_shape=(
            jax.ShapeDtypeStruct((strips, CORES, tokens, width), bf16),
            jax.ShapeDtypeStruct((strips, levels, CORES, 2, tokens, HEAD_SIZE), bf16),
            jax.ShapeDtypeStruct((strips, levels, CORES, 1, CORES * tokens), jnp.int32),
        ),
        in_specs=[anywhere, anywhere, anywhere, vmem],
        out_specs=(vmem, vmem, vmem),
        scratch_shapes=[(
            dma((4, slots)), dma((4, slots)),
            dma((strips + 1, levels, 2)), dma((strips + 1, levels)), dma((4,)),
        )],
        compiler_params=pltpu.CompilerParams(collective_id=0, has_side_effects=True),
    )(queries, key_rows, value_matrix, doc_row)
    docs = docs.reshape(sequence // tokens, 1, CORES * tokens)
    span = 2 * CORES * tokens
    attended = pl.pallas_call(
        functools.partial(attend_kernel, levels, heads, tokens, span),
        name="attend",
        out_shape=jax.ShapeDtypeStruct((strips, CORES, tokens, width), bf16),
        in_specs=[pl.BlockSpec(memory_space=pltpu.SMEM), vmem, vmem, vmem],
        out_specs=vmem,
        scratch_shapes=[
            pltpu.VMEM((heads // 2, HEAD_SIZE, 2 * CORES * tokens), jnp.float32),
            pltpu.VMEM((heads // 2, span, 2 * CORES * tokens), jnp.float32),
            pltpu.VMEM((heads // 2, span, 2 * CORES * tokens), bf16),
        ],
    )(
        docs.reshape(sequence // tokens, CORES * tokens),
        query_block,
        key_value.reshape(sequence // tokens, 2, tokens, HEAD_SIZE),
        docs,
    )
    return pl.pallas_call(
        functools.partial(return_kernel, slots),
        name="give_back",
        out_shape=jax.ShapeDtypeStruct((tokens, columns), bf16),
        in_specs=[vmem],
        out_specs=anywhere,
        scratch_shapes=[dma((slots,)), dma((slots,)), dma],
        compiler_params=pltpu.CompilerParams(collective_id=1, has_side_effects=True),
    )(attended)


def solution(mesh):
    rows = P(("kv", "head"), None)
    return jax.shard_map(
        functools.partial(local, mesh.shape["kv"], mesh.shape["head"] // CORES),
        mesh=mesh,
        in_specs=(rows, rows, rows, P(("kv", "head"))),
        out_specs=rows,
        check_vma=False,
    )
```

```python
import functools
import math

import jax
import jax.numpy as jnp
from jax import lax
from jax.experimental import pallas as pl
from jax.experimental.pallas import tpu as pltpu
from jax.sharding import PartitionSpec as P

QUERY_HEADS = 64
KEY_VALUE_HEADS = 8
HEAD_SIZE = 128
CORES = 2
NEG_FILL = -1e30
SCALE_LOG2 = HEAD_SIZE ** -0.5 * math.log2(math.e)
MESH = pl.DeviceIdType.MESH


def peer_id(slot, level):
    return {"kv": slot // CORES, "head": level * CORES + slot % CORES}


def order(slots):
    return sorted(range(1, slots), key=lambda step: (bin(step // CORES).count("1"), step))


def place():
    kv_here, head_here = lax.axis_index("kv"), lax.axis_index("head")
    return kv_here, head_here // CORES, lax.rem(head_here, CORES)


def gather_kernel(slots, levels, q_ref, k_ref, v_ref, d_ref, qo, kvo, do, sems):
    kv_here, level, core = place()
    me = kv_here * CORES + core
    width = q_ref.shape[1] // slots
    query_heads = width // HEAD_SIZE
    group = QUERY_HEADS // KEY_VALUE_HEADS
    slab_send, slab_recv, line_send, line_recv, own = sems

    barrier = pltpu.get_barrier_semaphore()
    for step in range(1, slots):
        peer = lax.rem(me + step, slots)
        pl.semaphore_signal(barrier, inc=1, device_id=peer_id(peer, level), device_id_type=MESH)

    @pl.when(level > 0)
    def _():
        pl.semaphore_signal(barrier, inc=1, device_id=peer_id(me, level - 1), device_id_type=MESH)

    @pl.when(level < levels - 1)
    def _():
        pl.semaphore_signal(barrier, inc=1, device_id=peer_id(me, level + 1), device_id_type=MESH)

    def parts(slot):
        kv_column = pl.multiple_of((slot * query_heads // group) * HEAD_SIZE, HEAD_SIZE)
        q_column = pl.multiple_of(slot * width, HEAD_SIZE)
        return (
            (k_ref.at[:, pl.ds(kv_column, HEAD_SIZE)], kvo.at[kv_here, level, core, 0]),
            (v_ref.at[:, pl.ds(kv_column, HEAD_SIZE)], kvo.at[kv_here, level, core, 1]),
            (d_ref, do.at[kv_here, level, core]),
            (q_ref.at[:, pl.ds(q_column, width)], qo.at[kv_here, core]),
        )

    local = [pltpu.make_async_copy(s, d, own.at[i]) for i, (s, d) in enumerate(parts(me))]
    for copy in local:
        copy.start()
    pl.semaphore_wait(
        barrier,
        slots - 1 + (level > 0).astype(jnp.int32) + (level < levels - 1).astype(jnp.int32),
    )

    def slab_copy(step, part):
        peer = me ^ step
        source, target = parts(peer)[part]
        return pltpu.make_async_remote_copy(
            src_ref=source, dst_ref=target,
            send_sem=slab_send.at[part, peer], recv_sem=slab_recv.at[part, me],
            device_id=peer_id(peer, level), device_id_type=MESH,
        )

    for part in range(4):
        for step in order(slots):
            slab_copy(step, part).start()

    def slab_wait(part, source):
        target = (
            kvo.at[source // CORES, level, lax.rem(source, CORES), 0],
            kvo.at[source // CORES, level, lax.rem(source, CORES), 1],
            do.at[source // CORES, level, lax.rem(source, CORES)],
            qo.at[source // CORES, lax.rem(source, CORES)],
        )[part]
        pltpu.make_async_remote_copy(
            src_ref=target, dst_ref=target,
            send_sem=slab_send.at[part, source], recv_sem=slab_recv.at[part, source],
            device_id=peer_id(source, level), device_id_type=MESH,
        ).wait_recv()

    strips = slots // CORES

    def line_copy(item, slab, up):
        whole = isinstance(item, int) and item == strips
        ref = do.at[:, slab] if whole else kvo.at[item, slab]
        return pltpu.make_async_remote_copy(
            src_ref=ref, dst_ref=ref,
            send_sem=line_send.at[item, slab, 1 if up else 0],
            recv_sem=line_recv.at[item, slab],
            device_id=peer_id(me, level + 1 if up else level - 1), device_id_type=MESH,
        )

    for copy in local:
        copy.wait()

    def both_ways(item):
        @pl.when(level < levels - 1)
        def _():
            line_copy(item, level, True).start()

        @pl.when(level > 0)
        def _():
            line_copy(item, level, False).start()

    for ahead in range(strips):
        strip = kv_here ^ ahead
        for source_core in range(CORES):
            source = strip * CORES + source_core

            @pl.when(source != me)
            def _():
                for part in range(2):
                    slab_wait(part, source)

        both_ways(strip)
    for step in range(1, slots):
        slab_wait(2, me ^ step)
    both_ways(strips)

    def passes(step):
        for up in (True, False):
            slab = level - step if up else level + step
            exists = (slab >= 0) if up else (slab < levels)
            onward = (level < levels - 1) if up else (level > 0)
            yield up, slab, exists, exists & onward

    for step in range(1, levels):
        for ahead in range(strips + 1):
            item = kv_here ^ ahead if ahead < strips else strips
            for up, slab, exists, onward in passes(step):
                @pl.when(exists)
                def _():
                    line_copy(item, slab, True).wait_recv()

                @pl.when(onward)
                def _():
                    line_copy(item, slab, up).start()

    for step in range(levels):
        for item in range(strips + 1):
            for up, slab, exists, onward in passes(step):
                @pl.when(onward)
                def _():
                    line_copy(item, slab, up).wait_send()

    for step in range(1, slots):
        slab_wait(3, lax.rem(me + step, slots))
    for part in range(4):
        for step in range(1, slots):
            slab_copy(step, part).wait_send()


def attend_kernel(levels, heads, tokens, span, docs_ref, q_ref, kv_ref, d_ref, o_ref, acc, held, rounded):
    strip = pl.program_id(0)
    rows = CORES * tokens
    level = lax.axis_index("head") // CORES
    pairs = heads // 2
    chunk = span // rows

    own_chunk = strip * levels + level
    first_doc = docs_ref[own_chunk * CORES, 0]
    high = own_chunk // chunk + 1

    def count(block, low):
        last = docs_ref[(block + 1) * chunk * CORES - 1, rows - 1]
        return low + jnp.where(last < first_doc, 1, 0)

    low = lax.fori_loop(0, high - 1, count, 0)
    acc[...] = jnp.zeros_like(acc)
    own_docs = d_ref[own_chunk * CORES] + d_ref[own_chunk * CORES + 1]
    query_pos = own_chunk * rows + lax.broadcasted_iota(jnp.int32, (span, rows), 1)

    def one_block(block, state):
        first = pl.multiple_of(block * span, span)
        pieces = pl.ds(block * chunk * CORES, chunk * CORES)
        keys = kv_ref[pieces, 0].reshape(span, HEAD_SIZE)
        values = kv_ref[pieces, 1].reshape(span, HEAD_SIZE).T
        key_docs = []
        for piece in range(chunk):
            at = (block * chunk + piece) * CORES
            key_docs.append(jnp.broadcast_to(d_ref[at] + d_ref[at + 1], (rows, rows)).T)
        key_docs = jnp.concatenate(key_docs, axis=0)
        key_pos = first + lax.broadcasted_iota(jnp.int32, (span, rows), 0)
        allowed = (key_docs == own_docs) & (key_pos <= query_pos)
        bias = jnp.where(allowed, 0.0, NEG_FILL)
        bias = jnp.concatenate([bias, bias], axis=1)
        peaks, totals = [], []

        def score(pair):
            queries = jnp.concatenate(
                [
                    q_ref[0, core, :, h * HEAD_SIZE:(h + 1) * HEAD_SIZE]
                    for h in (2 * pair, 2 * pair + 1)
                    for core in range(CORES)
                ],
                axis=0,
            )
            scores = lax.dot_general(
                keys, queries, (((1,), (1,)), ((), ())), preferred_element_type=jnp.float32
            ) + bias
            held[pair] = scores
            peaks.append(
                jnp.maximum(state[0][pair], jnp.max(scores, axis=0, keepdims=True))
            )

        def weigh(pair):
            peak = peaks[pair]
            weights = jnp.exp2((held[pair] - peak) * SCALE_LOG2)
            factor = jnp.exp2((state[0][pair] - peak) * SCALE_LOG2)
            totals.append(
                state[1][pair] * factor + jnp.sum(weights, axis=0, keepdims=True)
            )
            rounded[pair] = weights.astype(jnp.bfloat16)
            factors.append(factor)

        def fold(pair):
            acc[pair] = acc[pair] * factors[pair] + lax.dot_general(
                values, rounded[pair], (((1,), (0,)), ((), ())),
                preferred_element_type=jnp.float32,
            )

        factors = []
        score(0)
        for pair in range(pairs):
            if pair + 1 < pairs:
                score(pair + 1)
            weigh(pair)
            if pair >= 1:
                fold(pair - 1)
        fold(pairs - 1)
        return tuple(peaks), tuple(totals)

    start = (
        tuple(jnp.full((1, 2 * rows), NEG_FILL, jnp.float32) for _ in range(pairs)),
        tuple(jnp.zeros((1, 2 * rows), jnp.float32) for _ in range(pairs)),
    )
    _, totals = lax.fori_loop(low, high, one_block, start)
    for pair in range(pairs):
        result = acc[pair] / totals[pair]
        for half in range(2):
            head = 2 * pair + half
            turned = result[:, half * rows:(half + 1) * rows].T.astype(jnp.bfloat16)
            for core in range(CORES):
                o_ref[0, core, :, head * HEAD_SIZE:(head + 1) * HEAD_SIZE] = turned[
                    core * tokens:(core + 1) * tokens
                ]


def return_kernel(slots, a_ref, o_ref, send, recv, own):
    kv_here, level, core = place()
    me = kv_here * CORES + core
    width = a_ref.shape[3]
    barrier = pltpu.get_barrier_semaphore()
    for step in range(1, slots):
        peer = lax.rem(me + step, slots)
        pl.semaphore_signal(barrier, inc=1, device_id=peer_id(peer, level), device_id_type=MESH)

    def target(slot):
        return o_ref.at[:, pl.ds(pl.multiple_of(slot * width, HEAD_SIZE), width)]

    local = pltpu.make_async_copy(a_ref.at[kv_here, core], target(me), own)
    local.start()
    pl.semaphore_wait(barrier, slots - 1)

    def copy(step):
        peer = me ^ step
        return pltpu.make_async_remote_copy(
            src_ref=a_ref.at[peer // CORES, lax.rem(peer, CORES)], dst_ref=target(me),
            send_sem=send.at[peer], recv_sem=recv.at[me],
            device_id=peer_id(peer, level), device_id_type=MESH,
        )

    for step in order(slots):
        copy(step).start()
    for step in range(1, slots):
        source = lax.rem(me + step, slots)
        pltpu.make_async_remote_copy(
            src_ref=target(source), dst_ref=target(source),
            send_sem=send.at[source], recv_sem=recv.at[source],
            device_id=peer_id(source, level), device_id_type=MESH,
        ).wait_recv()
    for step in range(1, slots):
        copy(step).wait_send()
    local.wait()


def local(strips, levels, queries, key_rows, value_matrix, doc_ids):
    slots = strips * CORES
    tokens, columns = queries.shape
    width = columns // slots
    heads = width // HEAD_SIZE
    sequence = tokens * slots * levels
    core = lax.rem(lax.axis_index("head"), CORES)
    doc_row = jnp.stack([doc_ids, doc_ids])
    doc_row = jnp.where(jnp.arange(CORES)[:, None] == core, doc_row, 0)
    doc_row = doc_row.reshape(1, CORES * tokens)
    vmem = pl.BlockSpec(memory_space=pltpu.VMEM)
    anywhere = pl.BlockSpec(memory_space=pl.ANY)
    bf16 = jnp.bfloat16
    dma = pltpu.SemaphoreType.DMA
    query_block, key_value, docs = pl.pallas_call(
        functools.partial(gather_kernel, slots, levels),
        name="gather",
        out_shape=(
            jax.ShapeDtypeStruct((strips, CORES, tokens, width), bf16),
            jax.ShapeDtypeStruct((strips, levels, CORES, 2, tokens, HEAD_SIZE), bf16),
            jax.ShapeDtypeStruct((strips, levels, CORES, 1, CORES * tokens), jnp.int32),
        ),
        in_specs=[anywhere, anywhere, anywhere, vmem],
        out_specs=(anywhere, vmem, vmem),
        scratch_shapes=[(
            dma((4, slots)), dma((4, slots)),
            dma((strips + 1, levels, 2)), dma((strips + 1, levels)), dma((4,)),
        )],
        compiler_params=pltpu.CompilerParams(collective_id=0, has_side_effects=True),
    )(queries, key_rows, value_matrix, doc_row)
    docs = docs.reshape(sequence // tokens, 1, CORES * tokens)
    span = 2 * CORES * tokens
    by_strip = pl.BlockSpec((1, CORES, tokens, width), lambda strip: (strip, 0, 0, 0))
    attended = pl.pallas_call(
        functools.partial(attend_kernel, levels, heads, tokens, span),
        name="attend",
        out_shape=jax.ShapeDtypeStruct((strips, CORES, tokens, width), bf16),
        grid=(strips,),
        in_specs=[pl.BlockSpec(memory_space=pltpu.SMEM), by_strip, vmem, vmem],
        out_specs=by_strip,
        scratch_shapes=[
            pltpu.VMEM((heads // 2, HEAD_SIZE, 2 * CORES * tokens), jnp.float32),
            pltpu.VMEM((heads // 2, span, 2 * CORES * tokens), jnp.float32),
            pltpu.VMEM((heads // 2, span, 2 * CORES * tokens), bf16),
        ],
    )(
        docs.reshape(sequence // tokens, CORES * tokens),
        query_block,
        key_value.reshape(sequence // tokens, 2, tokens, HEAD_SIZE),
        docs,
    )
    return pl.pallas_call(
        functools.partial(return_kernel, slots),
        name="give_back",
        out_shape=jax.ShapeDtypeStruct((tokens, columns), bf16),
        in_specs=[vmem],
        out_specs=anywhere,
        scratch_shapes=[dma((slots,)), dma((slots,)), dma],
        compiler_params=pltpu.CompilerParams(collective_id=1, has_side_effects=True),
    )(attended)


def solution(mesh):
    rows = P(("kv", "head"), None)
    return jax.shard_map(
        functools.partial(local, mesh.shape["kv"], mesh.shape["head"] // CORES),
        mesh=mesh,
        in_specs=(rows, rows, rows, P(("kv", "head"))),
        out_specs=rows,
        check_vma=False,
    )
```
